32 devices in a mesh: attn: 4 (over y, x), expert: 8 (over z, core).
Axes of the slice: x: 2, y: 2, z: 4, core: 2. Of those that a mesh axis runs over, the one named last changes fastest.
Arguments:
- tokens: bfloat16 [1024, 2880], P(('attn', 'expert')), may hold values from -6 to 6
- expert_ids: int32 [1024, 4], P(('attn', 'expert')), may hold values from 0 to 7, all different within a row; in each aligned block of 32 rows (0 to 31, 32 to 63, ...) at most 32 rows name the same one
- gate_probs: float32 [1024, 4], P(('attn', 'expert')), may hold values from 0.05 to 0.6
- shed_blocks: int32 [8], replicated, may hold values from 0 to 4, as said below
- partner: int32 [8], replicated, may hold values from 0 to 7, as said below
- gate_weight: bfloat16 [8, 2880, 2880], P('expert', None, 'attn'), may hold values from -0.109375 to 0.109375
- up_weight: bfloat16 [8, 2880, 2880], P('expert', None, 'attn'), may hold values from -0.109375 to 0.109375
- down_weight: bfloat16 [8, 2880, 2880], P('expert', 'attn'), may hold values from -0.109375 to 0.109375
Outputs:
- moe_out: bfloat16 [1024, 2880], P(('attn', 'expert'))
The draws below stay inside these ranges and needn't reach their ends.
Inputs may be any that keep to these rules, and one draw needn't show every extreme that they name: `expert_ids`: in the rows of one device, no expert is named by more than 32 rows; the 4 experts of a token differ. `shed_blocks`: some expert has exactly 4. partner pairs the experts: partner[partner[e]] = e and partner[e] != e.
All inputs are finite; a program needn't handle non-finite values.
Results may differ from the reference program's by a relative error of at most 0.0081.
Values may be sent and summed in bfloat16 or wider, within the bound.
A program may use at most 128 MiB of HBM per device.

```python
import math
import jax
import jax.numpy as jnp
import numpy as np
from jax import lax

D = 2880
FF = 2880
TOP = 4
SHED_MOST = 4
TOK_DEV = 32
TOKENS = 1024
EXPERTS = 8
MOST = 32
N_ATTN = 4


def draw_shed_blocks(key, part):
    first = jax.random.fold_in(key, 11)
    second = jax.random.fold_in(key, 12)
    values = jax.random.randint(first, (EXPERTS,), 0, SHED_MOST + 1).astype(jnp.int32)
    chosen = jax.random.randint(second, (), 0, EXPERTS)
    return values.at[chosen].set(SHED_MOST).astype(jnp.int32)


def draw_partner(key, part):
    shuffled = jax.random.permutation(jax.random.fold_in(key, 21), EXPERTS).astype(jnp.int32)
    left_side = shuffled[0::2]
    right_side = shuffled[1::2]
    paired = jnp.zeros((EXPERTS,), jnp.int32).at[left_side].set(right_side).at[right_side].set(left_side)
    return paired.astype(jnp.int32)


def block_scale(stream_key, shape, pieces, least, high):
    factor_of, own = 1.0, jax.random.fold_in(stream_key, 6)
    for dim, shards_of in pieces:
        draws = jnp.exp(jax.random.uniform(jax.random.fold_in(own, dim), (shards_of,), jnp.float32, least / len(pieces), high / len(pieces)))
        factor_of = factor_of * jnp.repeat(draws, shape[dim] // shards_of).reshape([-1 if axis == dim else 1 for axis in range(len(shape))])
    return factor_of


def routed_block(key, own, number, rows, number_of, top, most, skew):
    ranking = jax.random.permutation(key, number_of)
    heavy_load, common = load_shares(number_of, rows * top, most, skew, True), load_shares(number_of, rows * top, most, skew, False)
    places = jnp.arange(number_of)

    def named(lengths, rotation):
        used = int((lengths > 0).sum())
        fixed = max(1, used // 4)
        shifted = fixed + (places - fixed + rotation * (used - fixed)) % max(1, number_of - fixed)
        return jnp.zeros((number_of,), jnp.int32).at[ranking[jnp.where(places < fixed, places, shifted)]].set(jnp.asarray(lengths, jnp.int32))

    lengths = jnp.where(number % 4 == 0, named(heavy_load, number // 4), named(common, number - number // 4 - 1))
    mixed = jax.random.permutation(jax.random.fold_in(own, 3), number_of)
    source_of, receiver = mixed[0:number_of // 2 * 2:2], mixed[1:number_of // 2 * 2:2]
    margin = jnp.minimum(lengths[source_of] - 1, most - lengths[receiver]) // 2
    margin = jnp.where((source_of == ranking[0]) | (receiver == ranking[0]) | (lengths[receiver] == 0), 0, jnp.maximum(margin, 0))
    shifted = jax.random.randint(jax.random.fold_in(own, 4), (number_of // 2,), 0, 1 << 20) % (margin + 1)
    lengths = lengths.at[source_of].add(-shifted).at[receiver].add(shifted)
    labels = jnp.searchsorted(jnp.cumsum(lengths), jnp.arange(rows * top), side="right").astype(jnp.int32)
    listing = labels.reshape(top, rows).T
    listing = listing[jax.random.permutation(jax.random.fold_in(own, 1), rows)]
    rotation = jax.random.randint(jax.random.fold_in(own, 2), (rows, 1), 0, top)
    return jnp.take_along_axis(listing, (jnp.arange(top)[None, :] + rotation) % top, axis=1)


def load_shares(amount, total, reach, slope, full):
    portions = [(1 << 20) // math.isqrt(standing ** slope) + 1 for standing in range(1, amount + 1)]
    largest = reach if full else min(reach, max(-(-total // amount), total * portions[0] // sum(portions)))
    least = 1 if total - largest >= amount - 1 else 0
    holding, spare = [largest] + [least] * (amount - 1), total - largest - least * (amount - 1)
    while spare > 0:
        free = [i for i in range(1, amount) if holding[i] < largest] or [i for i in range(1, amount) if holding[i] < reach]
        pool, remaining = sum([portions[i] for i in free]), spare
        for i in free:
            addition = min(reach - holding[i], max(1, remaining * portions[i] // pool), spare)
            holding[i] = holding[i] + addition
            spare = spare - addition
    return np.array(holding)


def gaussian(key, extent, scale, most, cuts=(), kind=jnp.bfloat16):
    drawn = jax.random.normal(key, extent, jnp.float32) * scale
    if len(cuts) > 0:
        drawn = block_scale(key, extent, cuts, -0.22, 0.18) * drawn
    return jnp.clip(drawn, min=-most, max=most).astype(kind)


def setup_inputs(seed: int = 0) -> dict:
    streams_of = jax.random.split(jax.random.key(seed), 9)
    tokens = gaussian(streams_of[0], (TOKENS, D), 1.0, 6.0, ((0, 32),))
    expert_ids_keys = jax.random.split(jax.random.fold_in(streams_of[1], 1), TOKENS // TOK_DEV)
    expert_ids_turns = jax.random.permutation(jax.random.fold_in(streams_of[1], 3), TOKENS // TOK_DEV)
    expert_ids = jax.vmap(lambda own, number: routed_block(jax.random.fold_in(streams_of[1], 2), own, number, TOK_DEV, EXPERTS, TOP, MOST, 2))(expert_ids_keys, expert_ids_turns).reshape((TOKENS, TOP))
    gate_probs = jnp.clip(jnp.exp(math.log(0.6) - 2.4849067 * jax.random.uniform(streams_of[2], (TOKENS, TOP), jnp.float32) ** block_scale(streams_of[2], (TOKENS, TOP), ((0, 32),), -0.2, 0.2)), 0.05, 0.6)
    shed_blocks = draw_shed_blocks(jax.random.fold_in(streams_of[8], 71), 0)
    partner = draw_partner(jax.random.fold_in(streams_of[8], 71), 0)
    gate_weight = gaussian(streams_of[5], (EXPERTS, D, FF), D ** -0.5, 0.109375, ((0, 8), (2, 4)))
    up_weight = gaussian(streams_of[6], (EXPERTS, D, FF), D ** -0.5, 0.109375, ((0, 8), (2, 4)))
    down_weight = gaussian(streams_of[7], (EXPERTS, FF, D), FF ** -0.5, 0.109375, ((0, 8), (1, 4)))
    return {"tokens": tokens, "expert_ids": expert_ids, "gate_probs": gate_probs, "shed_blocks": shed_blocks, "partner": partner, "gate_weight": gate_weight, "up_weight": up_weight, "down_weight": down_weight}


SWISH_SCALE = 1.702


def activate(rows, gate_w, up_w):
    gate_part = jnp.dot(rows, gate_w, preferred_element_type=jnp.float32)
    up_part = jnp.dot(rows, up_w, preferred_element_type=jnp.float32)
    return (gate_part * jax.nn.sigmoid(SWISH_SCALE * gate_part) * (up_part + 1.0)).astype(jnp.bfloat16)


def reference(tokens, expert_ids, gate_probs, shed_blocks, partner, gate_weight, up_weight, down_weight):
    capacity = TOK_DEV * TOP * N_ATTN
    block_size = capacity // 8
    flat_ids = expert_ids.reshape(-1).astype(jnp.int32)
    onehot = (flat_ids[:, None] == jnp.arange(EXPERTS, dtype=jnp.int32)[None, :]).astype(jnp.int32)
    global_rank = jnp.sum((jnp.cumsum(onehot, axis=0) - onehot) * onehot, axis=1).astype(jnp.int32)
    limit = (capacity - block_size * shed_blocks[partner]).astype(jnp.int32)
    own_limit = limit[flat_ids]
    own_partner = partner[flat_ids].astype(jnp.int32)
    native = global_rank < own_limit
    borrowed = jnp.logical_and(jnp.logical_not(native), global_rank < own_limit + block_size * shed_blocks[flat_ids])
    target = jnp.where(native, flat_ids, jnp.where(borrowed, own_partner, -1)).astype(jnp.int32)
    slot_index = jnp.where(native, global_rank, limit[own_partner] + global_rank - own_limit).astype(jnp.int32)
    usable = target >= 0
    flat_index = jnp.where(usable, target * capacity + slot_index, EXPERTS * capacity).astype(jnp.int32)
    token_rows = jnp.repeat(tokens, TOP, axis=0)
    slot_rows = jnp.zeros((EXPERTS * capacity, D), jnp.bfloat16).at[flat_index].set(token_rows, mode="drop")
    slot_rows = slot_rows.reshape(EXPERTS, capacity, D)
    slot_place = jnp.arange(capacity, dtype=jnp.int32)

    def expert_layer(operands):
        rows, gate_w, up_w, down_w, other, bound = operands
        hidden_own = activate(rows, gate_w, up_w)
        hidden_other = activate(rows, gate_weight[other], up_weight[other])
        out_own = jnp.dot(hidden_own, down_w, preferred_element_type=jnp.float32)
        out_other = jnp.dot(hidden_other, down_weight[other], preferred_element_type=jnp.float32)
        keep = (slot_place < bound)[:, None]
        return jnp.where(keep, out_own, out_other).astype(jnp.bfloat16)

    expert_out = lax.map(expert_layer, (slot_rows, gate_weight, up_weight, down_weight, partner.astype(jnp.int32), limit))
    picked = expert_out.reshape(EXPERTS * capacity, D)[jnp.minimum(flat_index, EXPERTS * capacity - 1)]
    weights = jnp.where(usable, gate_probs.reshape(-1), 0.0).astype(jnp.float32)
    mixed = picked.astype(jnp.float32) * weights[:, None]
    return mixed.reshape(TOKENS, TOP, D).sum(axis=1).astype(jnp.bfloat16)
```

```python
import jax
import jax.numpy as jnp
from jax import lax
from jax.sharding import PartitionSpec as P

SHED_MOST = 4


SWISH_SCALE = 1.702


def lookup(table, indices):
    places = jnp.arange(table.shape[0], dtype=jnp.int32)
    return jnp.sum(jnp.where(indices[:, None] == places[None, :], table[None, :], 0), axis=1)


def row_weights(all_ids, all_probs, shed_blocks, partner, capacity, block_size):
    me = lax.axis_index("expert").astype(jnp.int32)
    named = all_ids == me
    mask = jnp.any(named, axis=1).astype(jnp.int32)
    rank = jnp.cumsum(mask) - mask
    other = lookup(partner, me[None])
    bound = (
        capacity - block_size * lookup(shed_blocks, other) + block_size * lookup(shed_blocks, me[None])
    )
    weight = jnp.sum(jnp.where(named, all_probs, 0.0), axis=1)
    return jnp.where(rank < bound, weight, 0.0)


def on_device(
    tokens, expert_ids, gate_probs, shed_blocks, partner, gate_weight, up_weight, down_weight
):
    tok_rows, model_width = tokens.shape
    top_count = expert_ids.shape[1]
    capacity = tok_rows * top_count * lax.axis_size("attn")
    block_size = capacity // 8
    both = ("attn", "expert")
    all_ids = lax.all_gather(expert_ids, both, axis=0, tiled=True)
    all_probs = lax.all_gather(gate_probs, both, axis=0, tiled=True)
    rows = lax.all_gather(tokens, both, axis=0, tiled=True)
    weight = row_weights(all_ids, all_probs, shed_blocks, partner, capacity, block_size)
    gate_part = jnp.dot(rows, gate_weight[0], preferred_element_type=jnp.float32)
    up_part = jnp.dot(rows, up_weight[0], preferred_element_type=jnp.float32)
    hidden = gate_part * jax.nn.sigmoid(SWISH_SCALE * gate_part) * (up_part + 1.0)
    hidden = (hidden * weight[:, None]).astype(jnp.bfloat16)
    share = jnp.dot(hidden, down_weight[0], preferred_element_type=jnp.float32).astype(jnp.bfloat16)
    share = lax.psum_scatter(share, "attn", scatter_dimension=0, tiled=True)
    return lax.psum_scatter(share, "expert", scatter_dimension=0, tiled=True)


def solution(mesh):
    in_specs = (
        P(("attn", "expert"), None),
        P(("attn", "expert"), None),
        P(("attn", "expert"), None),
        P(),
        P(),
        P("expert", None, "attn"),
        P("expert", None, "attn"),
        P("expert", "attn", None),
    )
    out_specs = P(("attn", "expert"), None)
    return jax.shard_map(
        on_device, mesh=mesh, in_specs=in_specs, out_specs=out_specs, check_vma=False
    )
```

```python
import functools

import jax
import jax.numpy as jnp
from jax import lax
from jax.experimental import pallas as pl
from jax.experimental.pallas import tpu as pltpu
from jax.sharding import PartitionSpec as P

SHED_MOST = 4


SWISH_SCALE = 1.702
LANES = 128
VMEM_BYTES = 60 * 2**20
MESH = pl.DeviceIdType.MESH

OWN_X, OWN_Y, OWN_C, FWD_Y, FWD_X, PASS_X, PASS_Y, PASS_D = range(8)
SUM_C, HALF_X, HALF_Y, FULL_X, FULL_Y, BACK_Z, OUT_Z = range(8, 15)
META_Z, META_A, META_C = range(15, 18)
KINDS = 18


def lookup(table, indices):
    places = jnp.arange(table.shape[0], dtype=jnp.int32)
    return jnp.sum(jnp.where(indices[:, None] == places[None, :], table[None, :], 0), axis=1)


def served_rows(shed_blocks, partner, capacity):
    me = lax.axis_index("expert").astype(jnp.int32)[None]
    other = lookup(partner, me)
    block_size = capacity // 8
    return capacity + block_size * (lookup(shed_blocks, me) - lookup(shed_blocks, other))


def activate(gate_part, up_part, weight):
    return (gate_part * jax.nn.sigmoid(SWISH_SCALE * gate_part) * (up_part + 1.0) * weight).astype(
        jnp.bfloat16
    )


def kernel(
    tokens,
    meta,
    bound,
    gate_hbm,
    up_hbm,
    down_hbm,
    out,
    x,
    m,
    wcol,
    part,
    core_in,
    total,
    half_in,
    full_in,
    z_out,
    z_in,
    kept,
    gate,
    up,
    down,
    send_sem,
    recv_sem,
    load_sem,
):
    planes = x.shape[0]
    rows, width = tokens.shape
    half = rows // 2
    top = meta.shape[0] // 2
    a = lax.axis_index("attn")
    e = lax.axis_index("expert")
    z, c = e // 2, e % 2

    def xor(value, bits):
        result = value
        for bit in (1, 2, 4, 8):
            if bits & bit:
                result = result + bit - 2 * bit * ((value // bit) % 2)
        return result

    xn, yn, dn = xor(a, 1), xor(a, 2), xor(a, 3)
    oc = 1 - c
    to_x, to_y, to_d, to_c = (xn, e), (yn, e), (dn, e), (a, z * 2 + oc)

    def plane(s):
        low = (z % 2 + s % 2) % 2
        high = (z // 2 + s // 2) % 2
        return high * 2 + low

    def copy(kind, s, src, dst, to):
        return pltpu.make_async_remote_copy(
            src_ref=src,
            dst_ref=dst,
            send_sem=send_sem.at[kind, s],
            recv_sem=recv_sem.at[kind, s],
            device_id=to,
            device_id_type=MESH,
        )

    def same(kind, s, ref, to):
        return copy(kind, s, ref, ref, to)

    lo, hi = pl.ds(0, half), pl.ds(half, half)

    def make(kind, s):
        p = plane(s)
        if kind == OUT_Z:
            return copy(kind, s, tokens, x.at[z, c, a], (a, p * 2 + c))
        if kind == OWN_X:
            return same(kind, s, x.at[p, c, a], to_x)
        if kind == OWN_Y:
            return same(kind, s, x.at[p, c, a], to_y)
        if kind == OWN_C:
            return same(kind, s, x.at[p, c, a], to_c)
        if kind == FWD_Y:
            return same(kind, s, x.at[p, c, xn, lo], to_y)
        if kind == FWD_X:
            return same(kind, s, x.at[p, c, yn, hi], to_x)
        if kind == PASS_X:
            return same(kind, s, x.at[p, c, xn], to_c)
        if kind == PASS_Y:
            return same(kind, s, x.at[p, c, yn], to_c)
        if kind == PASS_D:
            return same(kind, s, x.at[p, c, dn], to_c)
        if kind == SUM_C:
            return copy(kind, s, part.at[s, oc], core_in.at[s], to_c)
        if kind == HALF_X:
            return copy(kind, s, total.at[s, dn, lo], half_in.at[s, 0], to_x)
        if kind == HALF_Y:
            return copy(kind, s, total.at[s, dn, hi], half_in.at[s, 1], to_y)
        if kind == FULL_X:
            return copy(kind, s, total.at[s, xn], full_in.at[s, 0], to_x)
        if kind == FULL_Y:
            return copy(kind, s, total.at[s, yn], full_in.at[s, 1], to_y)
        if kind == BACK_Z:
            return copy(kind, s, z_out.at[s], z_in.at[s], (a, p * 2 + c))
        if kind == META_Z:
            return copy(kind, s, meta, m.at[a, z, c], (a, p * 2 + c))
        if kind == META_A:
            to = (to_x, to_x, to_y, to_d)[s]
            return same(kind, s, m.at[a, :, c], to)
        if kind == META_C:
            return same(kind, s, m.at[:, :, c], to_c)

    def start(s, *kinds):
        for kind in kinds:
            make(kind, s).start()

    def arrived(s, *kinds):
        for kind in kinds:
            make(kind, s).wait_recv()

    def sent(s, *kinds):
        for kind in kinds:
            make(kind, s).wait_send()

    def widen(ref):
        return ref[...].astype(jnp.float32)

    barrier = pltpu.get_barrier_semaphore()
    peers = [to_x, to_y, to_d, to_c] + [(a, plane(s) * 2 + c) for s in range(1, planes)]
    for peer in peers:
        pl.semaphore_signal(barrier, inc=1, device_id=peer, device_id_type=MESH)

    own = pltpu.make_async_copy(tokens, x.at[z, c, a], load_sem.at[3])
    own_meta = pltpu.make_async_copy(meta, m.at[a, z, c], load_sem.at[4])
    loads = [
        pltpu.make_async_copy(gate_hbm.at[0], gate, load_sem.at[0]),
        pltpu.make_async_copy(up_hbm.at[0], up, load_sem.at[1]),
        pltpu.make_async_copy(down_hbm.at[0], down, load_sem.at[2]),
    ]
    own.start()
    own_meta.start()
    for load in loads:
        load.start()
    pl.semaphore_wait(barrier, len(peers))

    for s in range(1, planes):
        start(s, META_Z)
    own.wait()
    own_meta.wait()
    start(0, OWN_X, OWN_Y, OWN_C)
    for s in range(1, planes):
        start(s, OUT_Z)

    def stage_own(s):
        arrived(s, OUT_Z)
        start(s, OWN_X, OWN_Y, OWN_C)

    def stage_forward(s):
        arrived(s, OWN_X)
        start(s, FWD_Y, PASS_X)
        arrived(s, OWN_Y)
        start(s, FWD_X, PASS_Y)

    for s in range(1, planes):
        arrived(s, META_Z)
    for s in range(1, 4):
        start(s, META_A)
    stage_forward(0)
    for s in range(1, 4):
        arrived(s, META_A)
    start(0, META_C)
    stage_own(1)
    arrived(0, META_C)

    def row_weights():
        table = m[...].reshape(m.shape[0] * m.shape[1] * m.shape[2], 2 * top, LANES)
        blocks = table.shape[0]
        named = table[:, :top, :] == e.astype(jnp.float32)
        mask = jnp.sum(jnp.where(named, 1.0, 0.0), axis=1)
        prob = jnp.sum(jnp.where(named, table[:, top:, :], 0.0), axis=1)
        mask16 = mask.astype(jnp.bfloat16)
        i = lax.broadcasted_iota(jnp.int32, (LANES, LANES), 0)
        j = lax.broadcasted_iota(jnp.int32, (LANES, LANES), 1)
        before = jnp.where(i < j, 1.0, 0.0).astype(jnp.bfloat16)
        inside = jnp.dot(mask16, before, preferred_element_type=jnp.float32)
        i = lax.broadcasted_iota(jnp.int32, (blocks, blocks), 0)
        j = lax.broadcasted_iota(jnp.int32, (blocks, blocks), 1)
        earlier = jnp.where(j < i, 1.0, 0.0).astype(jnp.bfloat16)
        ahead = jnp.dot(earlier, mask16, preferred_element_type=jnp.float32)
        rank = inside + jnp.sum(ahead, axis=1, keepdims=True)
        weight = jnp.where(rank < bound[...], prob, 0.0)
        i = lax.broadcasted_iota(jnp.int32, (rows, LANES), 0)
        j = lax.broadcasted_iota(jnp.int32, (rows, LANES), 1)
        for aa in range(m.shape[0]):
            for zz in range(m.shape[1]):
                for cc in range(2):
                    block = (aa * m.shape[1] + zz) * 2 + cc
                    spread = jnp.where(i == j, weight[block : block + 1, :], 0.0)
                    wcol[zz, cc, aa] = jnp.sum(spread, axis=1, keepdims=True)

    row_weights()
    for load in loads:
        load.wait()

    def compute(s):
        p = plane(s)
        count = 2 * m.shape[0] * rows
        xs = x[p].reshape(count, width)
        gate_part = jnp.dot(xs, gate[...], preferred_element_type=jnp.float32)
        up_part = jnp.dot(xs, up[...], preferred_element_type=jnp.float32)
        hidden = activate(gate_part, up_part, wcol[p].reshape(count, 1))
        step = 8 * LANES
        for first in range(0, width, step):
            cols = slice(first, min(first + step, width))
            share = jnp.dot(hidden, down[:, cols], preferred_element_type=jnp.float32)
            part[s, :, :, :, cols] = share.astype(jnp.bfloat16).reshape(
                2, m.shape[0], rows, cols.stop - cols.start
            )

    def body(t, carry):
        @pl.when(t < planes)
        def _():
            arrived(t, FWD_Y, FWD_X)
            start(t, PASS_D)
            arrived(t, OWN_C, PASS_X, PASS_Y, PASS_D)

        @pl.when(t + 2 < planes)
        def _():
            stage_own(t + 2)

        @pl.when(t < planes)
        def _():
            compute(t)
            start(t, SUM_C)

        @pl.when(t + 1 < planes)
        def _():
            stage_forward(t + 1)

        @pl.when(t < planes)
        def _():
            arrived(t, SUM_C)
            total[t] = (widen(part.at[t, c]) + widen(core_in.at[t])).astype(jnp.bfloat16)
            start(t, HALF_X, HALF_Y)

        @pl.when(jnp.logical_and(t >= 1, t < planes + 1))
        def _():
            s = t - 1
            arrived(s, HALF_X, HALF_Y)
            low = widen(total.at[s, yn, lo]) + widen(half_in.at[s, 0])
            total[s, yn, lo] = low.astype(jnp.bfloat16)
            start(s, FULL_Y)
            high = widen(total.at[s, xn, hi]) + widen(half_in.at[s, 1])
            total[s, xn, hi] = high.astype(jnp.bfloat16)
            start(s, FULL_X)

        @pl.when(t >= 2)
        def _():
            s = t - 2
            arrived(s, FULL_X, FULL_Y)
            value = widen(total.at[s, a]) + widen(full_in.at[s, 0]) + widen(full_in.at[s, 1])

            @pl.when(s == 0)
            def _():
                kept[...] = value

            @pl.when(s > 0)
            def _():
                z_out[s] = value.astype(jnp.bfloat16)
                start(s, BACK_Z)

        return carry

    lax.fori_loop(0, planes + 2, body, 0)

    value = kept[...]
    for s in range(1, planes):
        arrived(s, BACK_Z)
        value = value + widen(z_in.at[s])
    out[...] = value.astype(out.dtype)

    def drain(s, carry):
        sent(s, *range(OWN_X, BACK_Z))

        @pl.when(s > 0)
        def _():
            sent(s, BACK_Z, OUT_Z, META_Z)

        return carry

    lax.fori_loop(0, planes, drain, 0)
    for s in range(1, 4):
        sent(s, META_A)
    sent(0, META_C)


def fused_bytes(group_count, planes, rows, width, hidden):
    wide = -(-width // LANES) * LANES
    block = rows * wide * 2
    weights = 2 * width * (-(-hidden // LANES) * LANES) * 2 + hidden * wide * 2
    return weights + planes * group_count * block * (2 + 2 + 1 + 1 + 2) + 12 * 2**20


def fused(tokens, meta, bound, gate_weight, up_weight, down_weight, group_count, planes):
    rows, width = tokens.shape
    hidden = gate_weight.shape[2]
    bf16, f32 = jnp.bfloat16, jnp.float32
    vmem = pl.BlockSpec(memory_space=pltpu.VMEM)
    hbm = pl.BlockSpec(memory_space=pl.ANY)
    return pl.pallas_call(
        kernel,
        out_shape=jax.ShapeDtypeStruct((rows, width), bf16),
        in_specs=[vmem, vmem, vmem, hbm, hbm, hbm],
        out_specs=vmem,
        scratch_shapes=[
            pltpu.VMEM((planes, 2, group_count, rows, width), bf16),
            pltpu.VMEM((group_count, planes, 2) + meta.shape, f32),
            pltpu.VMEM((planes, 2, group_count, rows, 1), f32),
            pltpu.VMEM((planes, 2, group_count, rows, width), bf16),
            pltpu.VMEM((planes, group_count, rows, width), bf16),
            pltpu.VMEM((planes, group_count, rows, width), bf16),
            pltpu.VMEM((planes, 2, rows // 2, width), bf16),
            pltpu.VMEM((planes, 2, rows, width), bf16),
            pltpu.VMEM((planes, rows, width), bf16),
            pltpu.VMEM((planes, rows, width), bf16),
            pltpu.VMEM((rows, width), f32),
            pltpu.VMEM((width, hidden), bf16),
            pltpu.VMEM((width, hidden), bf16),
            pltpu.VMEM((hidden, width), bf16),
            pltpu.SemaphoreType.DMA((KINDS, planes)),
            pltpu.SemaphoreType.DMA((KINDS, planes)),
            pltpu.SemaphoreType.DMA((5,)),
        ],
        compiler_params=pltpu.CompilerParams(
            collective_id=0, has_side_effects=True, vmem_limit_bytes=VMEM_BYTES
        ),
    )(tokens, meta, bound, gate_weight, up_weight, down_weight)


def gathered(tokens, expert_ids, gate_probs, bound, gate_weight, up_weight, down_weight):
    both = ("attn", "expert")
    all_ids = lax.all_gather(expert_ids, both, axis=0, tiled=True)
    all_probs = lax.all_gather(gate_probs, both, axis=0, tiled=True)
    rows = lax.all_gather(tokens, both, axis=0, tiled=True)
    named = all_ids == lax.axis_index("expert").astype(jnp.int32)
    mask = jnp.any(named, axis=1).astype(jnp.int32)
    rank = jnp.cumsum(mask) - mask
    weight = jnp.sum(jnp.where(named, all_probs, 0.0), axis=1)
    weight = jnp.where(rank < bound, weight, 0.0)
    gate_part = jnp.dot(rows, gate_weight[0], preferred_element_type=jnp.float32)
    up_part = jnp.dot(rows, up_weight[0], preferred_element_type=jnp.float32)
    hidden = activate(gate_part, up_part, weight[:, None])
    share = jnp.dot(hidden, down_weight[0], preferred_element_type=jnp.float32).astype(jnp.bfloat16)
    share = lax.psum_scatter(share, "attn", scatter_dimension=0, tiled=True)
    return lax.psum_scatter(share, "expert", scatter_dimension=0, tiled=True)


def on_device(
    tokens, expert_ids, gate_probs, shed_blocks, partner, gate_weight, up_weight, down_weight
):
    rows, width = tokens.shape
    group_count, expert_count = lax.axis_size("attn"), lax.axis_size("expert")
    top_count = expert_ids.shape[1]
    planes = expert_count // 2
    bound = served_rows(shed_blocks, partner, rows * top_count * group_count)
    fits = fused_bytes(group_count, planes, rows, width, gate_weight.shape[2]) <= VMEM_BYTES
    if group_count != 4 or planes != 4 or rows % 32 or rows > LANES or not fits:
        return gathered(
            tokens, expert_ids, gate_probs, bound, gate_weight, up_weight, down_weight
        )
    ids = jnp.pad(
        expert_ids.T.astype(jnp.float32), ((0, 0), (0, LANES - rows)), constant_values=-1.0
    )
    probs = jnp.pad(gate_probs.T, ((0, 0), (0, LANES - rows)))
    meta = jnp.concatenate([ids, probs], axis=0)
    bound = jnp.broadcast_to(bound.astype(jnp.float32)[:, None], (1, LANES))
    return fused(
        tokens, meta, bound, gate_weight, up_weight, down_weight, group_count, planes
    )


def solution(mesh):
    in_specs = (
        P(("attn", "expert"), None),
        P(("attn", "expert"), None),
        P(("attn", "expert"), None),
        P(),
        P(),
        P("expert", None, "attn"),
        P("expert", None, "attn"),
        P("expert", "attn", None),
    )
    out_specs = P(("attn", "expert"), None)
    return jax.shard_map(
        on_device, mesh=mesh, in_specs=in_specs, out_specs=out_specs, check_vma=False
    )
```

```python
import jax
import jax.numpy as jnp
from jax import lax
from jax.experimental import pallas as pl
from jax.experimental.pallas import tpu as pltpu
from jax.sharding import PartitionSpec as P

SHED_MOST = 4


SWISH_SCALE = 1.702
LANES = 128
VMEM_BYTES = 60 * 2**20
MESH = pl.DeviceIdType.MESH

OWN_X, OWN_Y, OWN_C, FWD_Y, FWD_X, PASS_X, PASS_Y, PASS_D = range(8)
SUM_C, HALF_X, HALF_Y, FULL_X, FULL_Y, BACK_Z, OUT_Z = range(8, 15)
META_Z, META_A, META_C = range(15, 18)
KINDS = 18


def lookup(table, indices):
    places = jnp.arange(table.shape[0], dtype=jnp.int32)
    return jnp.sum(jnp.where(indices[:, None] == places[None, :], table[None, :], 0), axis=1)


def served_rows(shed_blocks, partner, capacity):
    me = lax.axis_index("expert").astype(jnp.int32)[None]
    other = lookup(partner, me)
    block_size = capacity // 8
    return capacity + block_size * (lookup(shed_blocks, me) - lookup(shed_blocks, other))


def activate(gate_part, up_part, weight):
    return (gate_part * jax.nn.sigmoid(SWISH_SCALE * gate_part) * (up_part + 1.0) * weight).astype(
        jnp.bfloat16
    )


def kernel(
    tokens,
    ids,
    probs,
    shed,
    partner,
    gate_hbm,
    up_hbm,
    down_hbm,
    out,
    x,
    meta,
    m,
    wcol,
    part,
    core_in,
    total,
    half_in,
    full_in,
    z_out,
    z_in,
    kept,
    gate,
    up,
    down,
    hidden,
    send_sem,
    recv_sem,
    load_sem,
):
    planes = x.shape[0]
    rows, width = tokens.shape
    half = rows // 2
    top = ids.shape[0]
    capacity = rows * top * x.shape[2]
    a = lax.axis_index("attn")
    e = lax.axis_index("expert")
    z, c = e // 2, e % 2

    def xor(value, bits):
        result = value
        for bit in (1, 2, 4, 8):
            if bits & bit:
                result = result + bit - 2 * bit * ((value // bit) % 2)
        return result

    xn, yn, dn = xor(a, 1), xor(a, 2), xor(a, 3)
    oc = 1 - c
    to_x, to_y, to_d, to_c = (xn, e), (yn, e), (dn, e), (a, z * 2 + oc)

    def plane(s):
        low = (z % 2 + s % 2) % 2
        high = (z // 2 + s // 2) % 2
        return high * 2 + low

    def copy(kind, s, src, dst, to):
        return pltpu.make_async_remote_copy(
            src_ref=src,
            dst_ref=dst,
            send_sem=send_sem.at[kind, s],
            recv_sem=recv_sem.at[kind, s],
            device_id=to,
            device_id_type=MESH,
        )

    def same(kind, s, ref, to):
        return copy(kind, s, ref, ref, to)

    lo, hi = pl.ds(0, half), pl.ds(half, half)

    def make(kind, s):
        p = plane(s)
        if kind == OUT_Z:
            return copy(kind, s, tokens, x.at[z, c, a], (a, p * 2 + c))
        if kind == OWN_X:
            return same(kind, s, x.at[p, c, a], to_x)
        if kind == OWN_Y:
            return same(kind, s, x.at[p, c, a], to_y)
        if kind == OWN_C:
            return same(kind, s, x.at[p, c, a], to_c)
        if kind == FWD_Y:
            return same(kind, s, x.at[p, c, xn, lo], to_y)
        if kind == FWD_X:
            return same(kind, s, x.at[p, c, yn, hi], to_x)
        if kind == PASS_X:
            return same(kind, s, x.at[p, c, xn], to_c)
        if kind == PASS_Y:
            return same(kind, s, x.at[p, c, yn], to_c)
        if kind == PASS_D:
            return same(kind, s, x.at[p, c, dn], to_c)
        if kind == SUM_C:
            return copy(kind, s, part.at[s, oc], core_in.at[s], to_c)
        if kind == HALF_X:
            return copy(kind, s, total.at[s, dn, lo], half_in.at[s, 0], to_x)
        if kind == HALF_Y:
            return copy(kind, s, total.at[s, dn, hi], half_in.at[s, 1], to_y)
        if kind == FULL_X:
            return copy(kind, s, total.at[s, xn], full_in.at[s, 0], to_x)
        if kind == FULL_Y:
            return copy(kind, s, total.at[s, yn], full_in.at[s, 1], to_y)
        if kind == BACK_Z:
            return copy(kind, s, z_out.at[s], z_in.at[s], (a, p * 2 + c))
        if kind == META_Z:
            return copy(kind, s, meta, m.at[a, z, c], (a, p * 2 + c))
        if kind == META_A:
            to = (to_x, to_x, to_y, to_d)[s]
            return same(kind, s, m.at[a, :, c], to)
        if kind == META_C:
            return same(kind, s, m.at[:, :, c], to_c)

    def start(s, *kinds):
        for kind in kinds:
            make(kind, s).start()

    def arrived(s, *kinds):
        for kind in kinds:
            make(kind, s).wait_recv()

    def sent(s, *kinds):
        for kind in kinds:
            make(kind, s).wait_send()

    def widen(ref):
        return ref[...].astype(jnp.float32)

    barrier = pltpu.get_barrier_semaphore()
    peers = [to_x, to_y, to_d, to_c] + [(a, plane(s) * 2 + c) for s in range(1, planes)]
    for peer in peers:
        pl.semaphore_signal(barrier, inc=1, device_id=peer, device_id_type=MESH)

    own = pltpu.make_async_copy(tokens, x.at[z, c, a], load_sem.at[3])
    own_meta = pltpu.make_async_copy(meta, m.at[a, z, c], load_sem.at[4])
    loads = [
        pltpu.make_async_copy(gate_hbm.at[0], gate, load_sem.at[0]),
        pltpu.make_async_copy(up_hbm.at[0], up, load_sem.at[1]),
        pltpu.make_async_copy(down_hbm.at[0], down, load_sem.at[2]),
    ]
    own.start()
    meta[...] = jnp.full(meta.shape, -1.0, jnp.float32)
    meta[:top, :rows] = ids[...].astype(jnp.float32)
    meta[top:, :rows] = probs[...]
    for load in loads:
        load.start()
    pl.semaphore_wait(barrier, len(peers))

    for s in range(1, planes):
        start(s, META_Z)
    own_meta.start()
    own.wait()
    start(0, OWN_X, OWN_Y, OWN_C)
    for s in range(1, planes):
        start(s, OUT_Z)
    own_meta.wait()

    def stage_own(s):
        arrived(s, OUT_Z)
        start(s, OWN_X, OWN_Y, OWN_C)

    def stage_forward(s):
        arrived(s, OWN_X)
        start(s, FWD_Y, PASS_X)
        arrived(s, OWN_Y)
        start(s, FWD_X, PASS_Y)

    for s in range(1, planes):
        arrived(s, META_Z)
    for s in range(1, 4):
        start(s, META_A)
    stage_forward(0)
    for s in range(1, 4):
        arrived(s, META_A)
    start(0, META_C)
    stage_own(1)
    stage_own(2)
    arrived(0, META_C)

    def row_weights():
        table = m[...].reshape(m.shape[0] * m.shape[1] * m.shape[2], 2 * top, LANES)
        blocks = table.shape[0]
        named = table[:, :top, :] == e.astype(jnp.float32)
        mask = jnp.sum(jnp.where(named, 1.0, 0.0), axis=1)
        prob = jnp.sum(jnp.where(named, table[:, top:, :], 0.0), axis=1)
        mask16 = mask.astype(jnp.bfloat16)
        i = lax.broadcasted_iota(jnp.int32, (LANES, LANES), 0)
        j = lax.broadcasted_iota(jnp.int32, (LANES, LANES), 1)
        before = jnp.where(i < j, 1.0, 0.0).astype(jnp.bfloat16)
        inside = jnp.dot(mask16, before, preferred_element_type=jnp.float32)
        i = lax.broadcasted_iota(jnp.int32, (blocks, blocks), 0)
        j = lax.broadcasted_iota(jnp.int32, (blocks, blocks), 1)
        earlier = jnp.where(j < i, 1.0, 0.0).astype(jnp.bfloat16)
        ahead = jnp.dot(earlier, mask16, preferred_element_type=jnp.float32)
        rank = inside + jnp.sum(ahead, axis=1, keepdims=True)
        bound = capacity + capacity // 8 * (shed[e] - shed[partner[e]])
        weight = jnp.where(rank < bound.astype(jnp.float32), prob, 0.0)
        i = lax.broadcasted_iota(jnp.int32, (rows, LANES), 0)
        j = lax.broadcasted_iota(jnp.int32, (rows, LANES), 1)
        for aa in range(m.shape[0]):
            for zz in range(m.shape[1]):
                for cc in range(2):
                    block = (aa * m.shape[1] + zz) * 2 + cc
                    spread = jnp.where(i == j, weight[block : block + 1, :], 0.0)
                    wcol[zz, cc, aa] = jnp.sum(spread, axis=1, keepdims=True)

    row_weights()
    for load in loads:
        load.wait()
    stage_forward(1)

    count = 2 * x.shape[2] * rows
    along = (((1,), (1,)), ((), ()))

    def compute_hidden(s):
        p = plane(s)
        xs = x[p].reshape(count, width)
        gate_part = lax.dot_general(xs, gate[...], along, preferred_element_type=jnp.float32)
        up_part = lax.dot_general(xs, up[...], along, preferred_element_type=jnp.float32)
        hidden[...] = activate(gate_part, up_part, wcol[p].reshape(count, 1))

    def compute_share(s):
        step = 8 * LANES
        for first in range(0, width, step):
            cols = slice(first, min(first + step, width))
            share = jnp.dot(hidden[...], down[:, cols], preferred_element_type=jnp.float32)
            part[s, :, :, :, cols] = share.astype(jnp.bfloat16).reshape(
                2, x.shape[2], rows, cols.stop - cols.start
            )

    def order(t):
        return (t + 1) % planes

    def body(t, carry):
        @pl.when(t < planes)
        def _():
            s = order(t)
            arrived(s, FWD_Y, FWD_X)
            start(s, PASS_D)
            arrived(s, OWN_C, PASS_X, PASS_Y, PASS_D)

        @pl.when(t + 3 < planes)
        def _():
            stage_own(t + 3)

        @pl.when(t < planes)
        def _():
            compute_hidden(order(t))

        @pl.when(t + 2 < planes)
        def _():
            stage_forward(t + 2)

        @pl.when(jnp.logical_and(t >= 1, t < planes + 1))
        def _():
            s = order(t - 1)
            arrived(s, HALF_X, HALF_Y)
            low = widen(total.at[s, yn, lo]) + widen(half_in.at[s, 0])
            total[s, yn, lo] = low.astype(jnp.bfloat16)
            start(s, FULL_Y)
            high = widen(total.at[s, xn, hi]) + widen(half_in.at[s, 1])
            total[s, xn, hi] = high.astype(jnp.bfloat16)
            start(s, FULL_X)

        @pl.when(t < planes)
        def _():
            s = order(t)
            compute_share(s)
            start(s, SUM_C)
            arrived(s, SUM_C)
            total[s] = (widen(part.at[s, c]) + widen(core_in.at[s])).astype(jnp.bfloat16)
            start(s, HALF_X, HALF_Y)

        @pl.when(t >= 2)
        def _():
            s = order(t - 2)
            arrived(s, FULL_X, FULL_Y)
            value = widen(total.at[s, a]) + widen(full_in.at[s, 0]) + widen(full_in.at[s, 1])

            @pl.when(s == 0)
            def _():
                kept[...] = value

            @pl.when(s > 0)
            def _():
                z_out[s] = value.astype(jnp.bfloat16)
                start(s, BACK_Z)

        return carry

    lax.fori_loop(0, planes + 2, body, 0)

    value = kept[...]
    for s in range(1, planes):
        arrived(s, BACK_Z)
        value = value + widen(z_in.at[s])
    out[...] = value.astype(out.dtype)

    def drain(s, carry):
        sent(s, *range(OWN_X, BACK_Z))

        @pl.when(s > 0)
        def _():
            sent(s, BACK_Z, OUT_Z, META_Z)

        return carry

    lax.fori_loop(0, planes, drain, 0)
    for s in range(1, 4):
        sent(s, META_A)
    sent(0, META_C)


def fused_bytes(group_count, planes, rows, width, hidden):
    wide = -(-width // LANES) * LANES
    block = rows * wide * 2
    weights = 2 * width * (-(-hidden // LANES) * LANES) * 2 + hidden * wide * 2
    return weights + planes * group_count * block * (2 + 2 + 1 + 1 + 2) + 12 * 2**20


def fused(tokens, ids, probs, shed, partner, gate_weight, up_weight, down_weight, group_count, planes):
    rows, width = tokens.shape
    hidden = gate_weight.shape[1]
    count = 2 * group_count * rows
    table = (2 * ids.shape[0], LANES)
    bf16, f32 = jnp.bfloat16, jnp.float32
    vmem = pl.BlockSpec(memory_space=pltpu.VMEM)
    smem = pl.BlockSpec(memory_space=pltpu.SMEM)
    hbm = pl.BlockSpec(memory_space=pl.ANY)
    return pl.pallas_call(
        kernel,
        out_shape=jax.ShapeDtypeStruct((rows, width), bf16),
        in_specs=[vmem, vmem, vmem, smem, smem, hbm, hbm, hbm],
        out_specs=vmem,
        scratch_shapes=[
            pltpu.VMEM((planes, 2, group_count, rows, width), bf16),
            pltpu.VMEM(table, f32),
            pltpu.VMEM((group_count, planes, 2) + table, f32),
            pltpu.VMEM((planes, 2, group_count, rows, 1), f32),
            pltpu.VMEM((planes, 2, group_count, rows, width), bf16),
            pltpu.VMEM((planes, group_count, rows, width), bf16),
            pltpu.VMEM((planes, group_count, rows, width), bf16),
            pltpu.VMEM((planes, 2, rows // 2, width), bf16),
            pltpu.VMEM((planes, 2, rows, width), bf16),
            pltpu.VMEM((planes, rows, width), bf16),
            pltpu.VMEM((planes, rows, width), bf16),
            pltpu.VMEM((rows, width), f32),
            pltpu.VMEM((hidden, width), bf16),
            pltpu.VMEM((hidden, width), bf16),
            pltpu.VMEM((hidden, width), bf16),
            pltpu.VMEM((count, hidden), bf16),
            pltpu.SemaphoreType.DMA((KINDS, planes)),
            pltpu.SemaphoreType.DMA((KINDS, planes)),
            pltpu.SemaphoreType.DMA((5,)),
        ],
        compiler_params=pltpu.CompilerParams(
            collective_id=0, has_side_effects=True, vmem_limit_bytes=VMEM_BYTES
        ),
    )(tokens, ids, probs, shed, partner, gate_weight, up_weight, down_weight)


def gathered(tokens, expert_ids, gate_probs, bound, gate_weight, up_weight, down_weight):
    both = ("attn", "expert")
    all_ids = lax.all_gather(expert_ids, both, axis=0, tiled=True)
    all_probs = lax.all_gather(gate_probs, both, axis=0, tiled=True)
    rows = lax.all_gather(tokens, both, axis=0, tiled=True)
    named = all_ids == lax.axis_index("expert").astype(jnp.int32)
    mask = jnp.any(named, axis=1).astype(jnp.int32)
    rank = jnp.cumsum(mask) - mask
    weight = jnp.sum(jnp.where(named, all_probs, 0.0), axis=1)
    weight = jnp.where(rank < bound, weight, 0.0)
    gate_part = jnp.dot(rows, gate_weight[0], preferred_element_type=jnp.float32)
    up_part = jnp.dot(rows, up_weight[0], preferred_element_type=jnp.float32)
    hidden = activate(gate_part, up_part, weight[:, None])
    share = jnp.dot(hidden, down_weight[0], preferred_element_type=jnp.float32).astype(jnp.bfloat16)
    share = lax.psum_scatter(share, "attn", scatter_dimension=0, tiled=True)
    return lax.psum_scatter(share, "expert", scatter_dimension=0, tiled=True)


def on_device(
    tokens, expert_ids, gate_probs, shed_blocks, partner, gate_weight, up_weight, down_weight
):
    rows, width = tokens.shape
    group_count, expert_count = lax.axis_size("attn"), lax.axis_size("expert")
    top_count = expert_ids.shape[1]
    planes = expert_count // 2
    fits = fused_bytes(group_count, planes, rows, width, gate_weight.shape[2]) <= VMEM_BYTES
    if group_count != 4 or planes != 4 or rows % 32 or rows > LANES or not fits:
        bound = served_rows(shed_blocks, partner, rows * top_count * group_count)
        return gathered(
            tokens, expert_ids, gate_probs, bound, gate_weight, up_weight, down_weight
        )
    return fused(
        tokens,
        expert_ids.T,
        gate_probs.T,
        shed_blocks,
        partner,
        jnp.swapaxes(gate_weight, 1, 2),
        jnp.swapaxes(up_weight, 1, 2),
        down_weight,
        group_count,
        planes,
    )


def solution(mesh):
    in_specs = (
        P(("attn", "expert"), None),
        P(("attn", "expert"), None),
        P(("attn", "expert"), None),
        P(),
        P(),
        P("expert", None, "attn"),
        P("expert", None, "attn"),
        P("expert", "attn", None),
    )
    out_specs = P(("attn", "expert"), None)
    return jax.shard_map(
        on_device, mesh=mesh, in_specs=in_specs, out_specs=out_specs, check_vma=False
    )
```
